128 devices in a mesh: batch: 8 (over x, core), seq: 16 (over z, y).
Axes of the slice: x: 4, y: 4, z: 4, core: 2. Of those that a mesh axis runs over, the one named last changes fastest.
Arguments:
- query: bfloat16 [16, 64, 128], P('batch'), may hold values from -300 to 300
- cache_keys: bfloat16 [16, 32768, 512], P('batch', 'seq'), may hold values from -6 to 6
- cache_values: bfloat16 [16, 32768, 512], P('batch', 'seq'), may hold values from -6 to 6
- new_keys: bfloat16 [16, 512], P('batch'), may hold values from -6 to 6
- new_values: bfloat16 [16, 512], P('batch'), may hold values from -6 to 6
- key_up: bfloat16 [512, 1024], P('seq'), may hold values from -0.25 to 0.25
- value_up: bfloat16 [512, 1024], P('seq'), may hold values from -0.25 to 0.25
- out_weight: bfloat16 [8192, 8192], P('seq', 'batch'), may hold values from -0.5 to 0.5
- lengths: int32 [16], P('batch'), may hold values from 128 to 32768, as said below
Outputs:
- mixed: bfloat16 [16, 8192], P('seq', 'batch')
The draws below stay inside these ranges and needn't reach their ends.
Inputs may be any that keep to these rules, and one draw needn't show every extreme that they name: `lengths`: every length is a multiple of 128, at least 128; some sequence fills all 32768 slots. Slots at or beyond a sequence's length hold arbitrary finite entries that must not affect the result.
All inputs are finite; a program needn't handle non-finite values.
Results may differ from the reference program's by a relative error of at most 0.019.
Values may be sent and summed in bfloat16 or wider, within the bound.
No kernel may reach another device: no remote copies, remote signals or barrier semaphores. Data moves between devices by JAX's collectives and lax.ppermute only.
A program may use at most 64 MiB of HBM per device.

```python
import jax
import jax.numpy as jnp
from jax import lax

D = 8192
H = 64
KV = 8
DH = 128
R = 512
BLOCK = 128
BATCH = 16
NTOK = 32768


def draw_query(key, part):
    base = jax.random.truncated_normal(key, -5.0, 5.0, (BATCH, H, DH), jnp.float32)
    values = base * 2.25
    return values.astype(jnp.bfloat16)


def draw_lengths(key, part):
    blocks = NTOK // BLOCK
    counts = jax.random.randint(key, (BATCH,), 1, blocks + 1)
    filled = jax.random.randint(jax.random.fold_in(key, 3), (), 0, BATCH)
    counts = jnp.where(jnp.arange(BATCH) == filled, blocks, counts)
    return (counts * BLOCK).astype(jnp.int32)


def level_of(rng, extent, shards, least, largest):
    factor_of, own = 1.0, jax.random.fold_in(rng, 6)
    for axis_at, blocks in shards:
        heights = jnp.exp(jax.random.uniform(jax.random.fold_in(own, axis_at), (blocks,), jnp.float32, least / len(shards), largest / len(shards)))
        factor_of = factor_of * jnp.repeat(heights, extent[axis_at] // blocks).reshape([-1 if axis == axis_at else 1 for axis in range(len(extent))])
    return factor_of


def noise(stream_key, dims, deviation, reach, shards=(), held_as=jnp.bfloat16):
    drawn = deviation * jax.random.normal(stream_key, dims, jnp.float32)
    if shards:
        drawn = drawn * level_of(stream_key, dims, shards, -0.22, 0.18)
    return jnp.clip(drawn, -reach, reach).astype(held_as)


def setup_inputs(seed: int = 0) -> dict:
    key_of = jax.random.split(jax.random.key(seed), 10)
    query = draw_query(jax.random.fold_in(key_of[9], 71), 0)
    cache_keys = noise(key_of[1], (BATCH, NTOK, R), 1.0, 6.0, ((0, 8), (1, 16)))
    cache_values = noise(key_of[2], (BATCH, NTOK, R), 1.0, 6.0, ((0, 8), (1, 16)))
    new_keys = noise(key_of[3], (BATCH, R), 1.0, 6.0, ((0, 8),))
    new_values = noise(key_of[4], (BATCH, R), 1.0, 6.0, ((0, 8),))
    key_up = noise(key_of[5], (R, KV * DH), R ** -0.5, 0.25, ((0, 16),))
    value_up = noise(key_of[6], (R, KV * DH), R ** -0.5, 0.25, ((0, 16),))
    out_weight = noise(key_of[7], (H * DH, D), DH ** -0.5, 0.5, ((0, 16), (1, 8)))
    lengths = draw_lengths(jax.random.fold_in(key_of[9], 71), 0)
    return dict(query=query, cache_keys=cache_keys, cache_values=cache_values, new_keys=new_keys, new_values=new_values, key_up=key_up, value_up=value_up, out_weight=out_weight, lengths=lengths)


def reference(query, cache_keys, cache_values, new_keys, new_values, key_up, value_up, out_weight, lengths):
    highest = lax.Precision.HIGHEST
    key_wide = key_up.astype(jnp.float32).reshape(R, KV, DH)
    value_wide = value_up.astype(jnp.float32).reshape(R, KV, DH)
    score_scale_factor = DH ** -0.5
    positions = jnp.arange(NTOK, dtype=jnp.int32)

    def per_sequence(items):
        query_row, keys_row, values_row, new_key_row, new_value_row, length = items
        grouped = query_row.astype(jnp.float32).reshape(KV, H // KV, DH)
        query_latent = jnp.einsum("kgd,rkd->kgr", grouped, key_wide, precision=highest)
        scores = jnp.einsum("kgr,lr->kgl", query_latent, keys_row.astype(jnp.float32), precision=highest) * score_scale_factor
        live_slots = positions < length
        scores = jnp.where(live_slots[None, None, :], scores, -jnp.inf)
        fresh_key_row = jnp.einsum("r,rkd->kd", new_key_row.astype(jnp.float32), key_wide, precision=highest)
        new_value = jnp.einsum("r,rkd->kd", new_value_row.astype(jnp.float32), value_wide, precision=highest)
        current_token_score = jnp.einsum("kgd,kd->kg", grouped, fresh_key_row, precision=highest) * score_scale_factor
        upper_limit = jnp.maximum(jnp.max(scores, axis=-1), current_token_score)
        softmax_terms = jnp.exp(scores - upper_limit[..., None])
        own_weight = jnp.exp(current_token_score - upper_limit)
        denominator = jnp.sum(softmax_terms, axis=-1) + own_weight
        latent_sum = jnp.einsum("kgl,lr->kgr", softmax_terms, values_row.astype(jnp.float32), precision=highest)
        totals = jnp.einsum("kgr,rkd->kgd", latent_sum, value_wide, precision=highest)
        totals = totals + own_weight[..., None] * new_value[:, None, :]
        return (totals / denominator[..., None]).reshape(H * DH).astype(jnp.bfloat16)

    attended = lax.map(per_sequence, (query, cache_keys, cache_values, new_keys, new_values, lengths))
    return jnp.dot(attended, out_weight, preferred_element_type=jnp.float32).astype(jnp.bfloat16)
```

```python
import functools

import jax
import jax.numpy as jnp
from jax import lax
from jax.experimental import pallas as pl
from jax.experimental.pallas import tpu as pltpu
from jax.sharding import PartitionSpec as P

NEGATIVE = -1e30
FLOOR = -1e20
VMEM = pltpu.VMEM
MIB = 1024 * 1024


def iota(shape, dim):
    return lax.broadcasted_iota(jnp.int32, shape, dim)


def whole(n):
    return [pl.BlockSpec(memory_space=VMEM)] * n


def split(value):
    high = value.astype(jnp.bfloat16).astype(jnp.float32)
    return high, value - high


def latent_kernel(query_ref, key_up_ref, out_ref):
    peers, ranks, _ = out_ref.shape
    flat = query_ref[...].reshape(128, 128)
    row, col = iota((128, 128), 0), iota((128, 128), 1)
    source = ((row >> 2) & 1) * 64 + (row >> 3) * 4 + (row & 3)
    pick = jnp.where(col == source, 1.0, 0.0).astype(jnp.bfloat16)
    ordered = jnp.dot(pick, flat, preferred_element_type=jnp.float32)
    blocks = [
        jnp.where((row >> 4) == k, ordered, 0.0).astype(jnp.bfloat16) for k in range(8)
    ]
    latent = lax.dot_general(
        key_up_ref[...],
        jnp.concatenate(blocks, axis=1),
        (((1,), (1,)), ((), ())),
        preferred_element_type=jnp.float32,
    )
    high, low = split(latent)
    piece = jnp.concatenate([high, low], axis=1).astype(jnp.bfloat16)
    for k in range(peers):
        out_ref[k] = piece


def attend_kernel(
    scale,
    shift_ref,
    lengths_ref,
    latent_ref,
    keys_ref,
    values_ref,
    new_keys_ref,
    new_values_ref,
    value_up_ref,
    out_ref,
    scores_ref,
    weights_ref,
):
    peers, ranks, width = latent_ref.shape
    rank = peers * ranks
    length = keys_ref.shape[1]
    chunk = 512
    shift = shift_ref[0]
    both = latent_ref[...].reshape(rank, width)
    lane = iota((rank, width), 1)
    maps = [
        jnp.where(((lane >> 2) & 1) == b, both.astype(jnp.float32), 0.0).astype(jnp.bfloat16)
        for b in range(2)
    ]
    second = ((iota((1, 128), 1) >> 2) & 1) == 1
    limit = jnp.where(second, lengths_ref[1], lengths_ref[0]) - shift
    top = jnp.full((8, 128), FLOOR, jnp.float32)
    for c in range(length // chunk):
        at = pl.ds(c * chunk, chunk)
        raw = jnp.dot(keys_ref[0, at, :], maps[0], preferred_element_type=jnp.float32)
        raw += jnp.dot(keys_ref[1, at, :], maps[1], preferred_element_type=jnp.float32)
        scores = (raw[:, :128] + raw[:, 128:]) * scale
        live = iota((chunk, 128), 0) + c * chunk < limit
        scores = jnp.where(live, scores, NEGATIVE)
        scores_ref[at, :] = scores
        top = jnp.maximum(top, jnp.max(scores.reshape(chunk // 8, 8, 128), axis=0))
    fresh = jnp.dot(new_keys_ref[...], maps[0], preferred_element_type=jnp.float32)[0:1]
    fresh += jnp.dot(new_keys_ref[...], maps[1], preferred_element_type=jnp.float32)[1:2]
    fresh = (fresh[:, :128] + fresh[:, 128:]) * scale
    fresh = jnp.where(shift == 0, fresh, NEGATIVE)
    top = jnp.maximum(jnp.max(top, axis=0, keepdims=True), fresh)
    total = jnp.zeros((8, 128), jnp.float32)
    for c in range(length // chunk):
        at = pl.ds(c * chunk, chunk)
        weights = jnp.exp(scores_ref[at, :] - top)
        total += jnp.sum(weights.reshape(chunk // 8, 8, 128), axis=0)
        weights_ref[:, at] = weights.T.astype(jnp.bfloat16)
    own = jnp.exp(fresh - top)
    total = jnp.sum(total, axis=0, keepdims=True) + own
    top_high, rest = split(top)
    top_mid, top_low = split(rest)
    total_high, total_low = split(total)
    row = iota((128, 128), 0)
    table = jnp.zeros((128, 128), jnp.float32)
    for k, line in enumerate((top_high, top_mid, top_low, total_high, total_low, own)):
        table = jnp.where(row == k, line, table)
    table = table.T
    own_column = table[:, 5:6]
    sums = [
        jnp.dot(weights_ref[...], values_ref[b], preferred_element_type=jnp.float32)
        for b in range(2)
    ]
    fresh_values = new_values_ref[...].astype(jnp.float32)
    upper = ((iota((128, rank), 0) >> 2) & 1) == 1
    summed = jnp.where(upper, sums[1], sums[0]) + own_column * jnp.where(
        upper, fresh_values[1:2], fresh_values[0:1]
    )
    for k in range(peers):
        lines = summed[8 * k : 8 * k + 8]
        stack = [lines[:, 128 * g : 128 * g + 128] for g in range(rank // 128)]
        out_ref[k, 0:32, :] = jnp.concatenate(stack, axis=0).astype(jnp.bfloat16)
        out_ref[k, 32:64, :] = value_up_ref[:, 128 * (k // 2) : 128 * (k // 2) + 128]
        out_ref[k, 64:72, :] = table[8 * k : 8 * k + 8].astype(jnp.bfloat16)


def merge_kernel(parts_ref, out_ref):
    peers = parts_ref.shape[0]
    stats = parts_ref[:, 64:72, :].reshape(peers * 8, 128)
    row, col = iota((128, 256), 0), iota((128, 256), 1)
    pick = ((col < 128) & (row < 3)) | ((col >= 128) & ((row == 3) | (row == 4)))
    spread = jnp.dot(
        stats, jnp.where(pick, 1.0, 0.0).astype(jnp.bfloat16), preferred_element_type=jnp.float32
    )
    tops = [spread[8 * k : 8 * k + 8, :128] for k in range(peers)]
    top = functools.reduce(jnp.maximum, tops)
    total = jnp.zeros((8, 128), jnp.float32)
    sums = [jnp.zeros((8, 128), jnp.float32) for _ in range(4)]
    for k in range(peers):
        factor = jnp.exp(tops[k] - top)
        total += factor * spread[8 * k : 8 * k + 8, 128:]
        lines = parts_ref[k, 0:32, :].astype(jnp.float32)
        for g in range(4):
            sums[g] += factor * lines[8 * g : 8 * g + 8]
    latent = jnp.concatenate([s / total for s in sums], axis=1)
    high, low = split(latent)
    table = parts_ref[:, 32:64, :].reshape(peers * 32, 128)
    both = jnp.dot(
        jnp.concatenate([high, low], axis=0).astype(jnp.bfloat16),
        table,
        preferred_element_type=jnp.float32,
    )
    attended = (both[:8] + both[8:]).astype(jnp.bfloat16)
    for k in range(out_ref.shape[0]):
        out_ref[k] = attended


def project_kernel(attended_ref, weight_ref, out_ref):
    rows = attended_ref.shape[0] * attended_ref.shape[1]
    seqs = rows // 4
    flat = attended_ref[...].reshape(rows, 128)
    row, col = iota((rows, rows), 0), iota((rows, rows), 1)
    pick = jnp.where(col == (row % seqs) * 4 + row // seqs, 1.0, 0.0).astype(jnp.bfloat16)
    ordered = jnp.dot(pick, flat, preferred_element_type=jnp.float32)
    lines = jnp.concatenate([ordered[seqs * h : seqs * h + seqs] for h in range(4)], axis=1)
    mixed = jnp.dot(
        lines.astype(jnp.bfloat16), weight_ref[...], preferred_element_type=jnp.float32
    )
    for j in range(out_ref.shape[1]):
        out_ref[:, j, :] = mixed[:, 128 * j : 128 * j + 128]


def sum_kernel(parts_ref, out_ref):
    total = jnp.sum(parts_ref[...], axis=0).astype(jnp.bfloat16)
    for j in range(total.shape[0]):
        out_ref[0:1, 128 * j : 128 * j + 128] = total[j : j + 1]


def call(kernel, shape, dtype, count, scratch=(), specs=None, limit=8, flops=0, name=None):
    return pl.pallas_call(
        kernel,
        out_shape=jax.ShapeDtypeStruct(shape, dtype),
        in_specs=specs or whole(count),
        out_specs=pl.BlockSpec(memory_space=VMEM),
        scratch_shapes=list(scratch),
        compiler_params=pltpu.CompilerParams(vmem_limit_bytes=limit * MIB),
        name=name,
    )


def exchange(value, axis):
    return lax.all_to_all(value, axis, 0, 0, tiled=True)


def body(
    query, cache_keys, cache_values, new_keys, new_values, key_up, value_up, out_weight, lengths
):
    peers, groups = lax.axis_size("seq"), lax.axis_size("batch")
    length, rank = cache_keys.shape[1], cache_keys.shape[2]
    ranks, columns = key_up.shape[0], out_weight.shape[1]
    scale = query.shape[2] ** -0.5
    shift = (lax.axis_index("seq") * length).astype(jnp.int32).reshape(1)
    latent = call(latent_kernel, (peers, ranks, 256), jnp.bfloat16, 2, name="latent")(
        query, key_up
    )
    latent = exchange(latent, "seq")
    smem = [pl.BlockSpec(memory_space=pltpu.SMEM)] * 2
    parts = call(
        functools.partial(attend_kernel, scale),
        (peers, 72, 128),
        jnp.bfloat16,
        8,
        scratch=[VMEM((length, 128), jnp.float32), VMEM((128, length), jnp.bfloat16)],
        specs=smem + whole(6),
        limit=24,
        name="attend",
    )(shift, lengths, latent, cache_keys, cache_values, new_keys, new_values, value_up)
    parts = exchange(parts, "seq")
    attended = call(merge_kernel, (groups, 8, 128), jnp.bfloat16, 1, name="merge")(parts)
    attended = exchange(attended, "batch")
    mixed = call(project_kernel, (peers, columns // 128, 128), jnp.float32, 2, name="project")(
        attended, out_weight
    )
    mixed = exchange(mixed, "seq")
    return call(sum_kernel, (1, columns), jnp.bfloat16, 1, name="total")(mixed)


def solution(mesh):
    return jax.shard_map(
        body,
        mesh=mesh,
        in_specs=(
            P("batch", None, None),
            P("batch", "seq", None),
            P("batch", "seq", None),
            P("batch", None),
            P("batch", None),
            P("seq", None),
            P("seq", None),
            P("seq", "batch"),
            P("batch"),
        ),
        out_specs=P("seq", "batch"),
        check_vma=False,
    )
```

```python
import functools

import jax
import jax.numpy as jnp
from jax import lax
from jax.experimental import pallas as pl
from jax.experimental.pallas import tpu as pltpu
from jax.sharding import PartitionSpec as P

NEGATIVE = -1e30
FLOOR = -1e20
VMEM = pltpu.VMEM
MIB = 1024 * 1024
LEAD, LATENT = 2 * 10**10, 2 * 10**10


def iota(shape, dim):
    return lax.broadcasted_iota(jnp.int32, shape, dim)


def whole(n):
    return [pl.BlockSpec(memory_space=VMEM)] * n


def split(value):
    high = value.astype(jnp.bfloat16).astype(jnp.float32)
    return high, value - high


def lead_kernel(out_ref):
    out_ref[...] = jnp.zeros_like(out_ref)


def latent_kernel(lead_ref, query_ref, key_up_ref, out_ref):
    flat = query_ref[...].reshape(128, 128)
    row, col = iota((128, 128), 0), iota((128, 128), 1)
    source = ((row >> 2) & 1) * 64 + (row >> 3) * 4 + (row & 3)
    pick = jnp.where(col == source, 1.0, 0.0).astype(jnp.bfloat16)
    ordered = jnp.dot(pick, flat, preferred_element_type=jnp.float32)
    blocks = [
        jnp.where((row >> 4) == k, ordered, 0.0).astype(jnp.bfloat16) for k in range(8)
    ]
    latent = lax.dot_general(
        key_up_ref[...],
        jnp.concatenate(blocks, axis=1),
        (((1,), (1,)), ((), ())),
        preferred_element_type=jnp.float32,
    )
    high, low = split(latent)
    piece = jnp.concatenate([high, low], axis=1).astype(jnp.bfloat16)
    for k in range(out_ref.shape[0]):
        out_ref[k] = piece


def attend_kernel(
    scale,
    lengths_ref,
    latent_ref,
    keys_ref,
    values_ref,
    new_keys_ref,
    new_values_ref,
    value_up_ref,
    out_ref,
    scores_ref,
    weights_ref,
):
    peers, ranks, width = latent_ref.shape
    rank = peers * ranks
    length = keys_ref.shape[1]
    chunk = 512
    shift = lax.axis_index("seq") * length
    both = latent_ref[...].reshape(rank, width)
    lane = iota((rank, width), 1)
    maps = [
        jnp.where(((lane >> 2) & 1) == b, both.astype(jnp.float32), 0.0).astype(jnp.bfloat16)
        for b in range(2)
    ]
    second = ((iota((1, 128), 1) >> 2) & 1) == 1
    limit = jnp.where(second, lengths_ref[1], lengths_ref[0]) - shift
    top = jnp.full((8, 128), FLOOR, jnp.float32)
    for c in range(length // chunk):
        at = pl.ds(c * chunk, chunk)
        raw = jnp.dot(keys_ref[0, at, :], maps[0], preferred_element_type=jnp.float32)
        raw += jnp.dot(keys_ref[1, at, :], maps[1], preferred_element_type=jnp.float32)
        scores = (raw[:, :128] + raw[:, 128:]) * scale
        live = iota((chunk, 128), 0) + c * chunk < limit
        scores = jnp.where(live, scores, NEGATIVE)
        scores_ref[at, :] = scores
        top = jnp.maximum(top, jnp.max(scores.reshape(chunk // 8, 8, 128), axis=0))
    fresh = jnp.dot(new_keys_ref[...], maps[0], preferred_element_type=jnp.float32)[0:1]
    fresh += jnp.dot(new_keys_ref[...], maps[1], preferred_element_type=jnp.float32)[1:2]
    fresh = (fresh[:, :128] + fresh[:, 128:]) * scale
    fresh = jnp.where(shift == 0, fresh, NEGATIVE)
    top = jnp.maximum(jnp.max(top, axis=0, keepdims=True), fresh)
    total = jnp.zeros((8, 128), jnp.float32)
    for c in range(length // chunk):
        at = pl.ds(c * chunk, chunk)
        weights = jnp.exp(scores_ref[at, :] - top)
        total += jnp.sum(weights.reshape(chunk // 8, 8, 128), axis=0)
        weights_ref[:, at] = weights.T.astype(jnp.bfloat16)
    own = jnp.exp(fresh - top)
    total = jnp.sum(total, axis=0, keepdims=True) + own
    top_high, rest = split(top)
    top_mid, top_low = split(rest)
    total_high, total_low = split(total)
    row = iota((128, 128), 0)
    table = jnp.zeros((128, 128), jnp.float32)
    for k, line in enumerate((top_high, top_mid, top_low, total_high, total_low, own)):
        table = jnp.where(row == k, line, table)
    table = table.T
    own_column = table[:, 5:6]
    sums = [
        jnp.dot(weights_ref[...], values_ref[b], preferred_element_type=jnp.float32)
        for b in range(2)
    ]
    fresh_values = new_values_ref[...].astype(jnp.float32)
    upper = ((iota((128, rank), 0) >> 2) & 1) == 1
    summed = jnp.where(upper, sums[1], sums[0]) + own_column * jnp.where(
        upper, fresh_values[1:2], fresh_values[0:1]
    )
    for k in range(peers):
        lines = summed[8 * k : 8 * k + 8]
        stack = [lines[:, 128 * g : 128 * g + 128] for g in range(rank // 128)]
        out_ref[k, 0:32, :] = jnp.concatenate(stack, axis=0).astype(jnp.bfloat16)
        out_ref[k, 32:64, :] = value_up_ref[:, 128 * (k // 2) : 128 * (k // 2) + 128]
        out_ref[k, 64:72, :] = table[8 * k : 8 * k + 8].astype(jnp.bfloat16)


def merge_kernel(parts_ref, out_ref):
    peers = parts_ref.shape[0]
    stats = parts_ref[:, 64:72, :].reshape(peers * 8, 128)
    row, col = iota((128, 256), 0), iota((128, 256), 1)
    pick = ((col < 128) & (row < 3)) | ((col >= 128) & ((row == 3) | (row == 4)))
    spread = jnp.dot(
        stats, jnp.where(pick, 1.0, 0.0).astype(jnp.bfloat16), preferred_element_type=jnp.float32
    )
    tops = [spread[8 * k : 8 * k + 8, :128] for k in range(peers)]
    top = functools.reduce(jnp.maximum, tops)
    total = jnp.zeros((8, 128), jnp.float32)
    sums = [jnp.zeros((8, 128), jnp.float32) for _ in range(4)]
    for k in range(peers):
        factor = jnp.exp(tops[k] - top)
        total += factor * spread[8 * k : 8 * k + 8, 128:]
        lines = parts_ref[k, 0:32, :].astype(jnp.float32)
        for g in range(4):
            sums[g] += factor * lines[8 * g : 8 * g + 8]
    latent = jnp.concatenate([s / total for s in sums], axis=1)
    high, low = split(latent)
    table = parts_ref[:, 32:64, :].reshape(peers * 32, 128)
    both = jnp.dot(
        jnp.concatenate([high, low], axis=0).astype(jnp.bfloat16),
        table,
        preferred_element_type=jnp.float32,
    )
    attended = (both[:8] + both[8:]).astype(jnp.bfloat16)
    for k in range(out_ref.shape[0]):
        out_ref[k] = attended


def project_kernel(attended_ref, weight_ref, out_ref):
    rows = attended_ref.shape[0] * attended_ref.shape[1]
    seqs = rows // 4
    flat = attended_ref[...].reshape(rows, 128)
    row, col = iota((rows, rows), 0), iota((rows, rows), 1)
    pick = jnp.where(col == (row % seqs) * 4 + row // seqs, 1.0, 0.0).astype(jnp.bfloat16)
    ordered = jnp.dot(pick, flat, preferred_element_type=jnp.float32)
    lines = jnp.concatenate([ordered[seqs * h : seqs * h + seqs] for h in range(4)], axis=1)
    mixed = jnp.dot(
        lines.astype(jnp.bfloat16), weight_ref[...], preferred_element_type=jnp.float32
    )
    for j in range(out_ref.shape[1]):
        out_ref[:, j, :] = mixed[:, 128 * j : 128 * j + 128]


def sum_kernel(parts_ref, out_ref):
    total = jnp.sum(parts_ref[...], axis=0).astype(jnp.bfloat16)
    for j in range(total.shape[0]):
        out_ref[0:1, 128 * j : 128 * j + 128] = total[j : j + 1]


def call(kernel, outs, count, scratch=(), specs=None, limit=8, flops=0, name=None):
    outs = [jax.ShapeDtypeStruct(*out) for out in outs]
    one = len(outs) == 1
    return pl.pallas_call(
        kernel,
        out_shape=outs[0] if one else outs,
        in_specs=whole(count) if specs is None else specs,
        out_specs=whole(1)[0] if one else whole(len(outs)),
        scratch_shapes=list(scratch),
        compiler_params=pltpu.CompilerParams(vmem_limit_bytes=limit * MIB),
        cost_estimate=pl.CostEstimate(flops=flops, bytes_accessed=0, transcendentals=0),
        name=name,
    )


def exchange(value, axis):
    return lax.all_to_all(value, axis, 0, 0, tiled=True)


def body(
    query, cache_keys, cache_values, new_keys, new_values, key_up, value_up, out_weight, lengths
):
    peers, groups = lax.axis_size("seq"), lax.axis_size("batch")
    length, rank = cache_keys.shape[1], cache_keys.shape[2]
    ranks, columns = key_up.shape[0], out_weight.shape[1]
    scale = query.shape[2] ** -0.5
    f32, bf16 = jnp.float32, jnp.bfloat16
    lead = call(lead_kernel, [((8, 128), f32)], 0, limit=4, flops=LEAD, name="lead")()
    latent = call(
        latent_kernel, [((peers, ranks, 256), bf16)], 3, limit=4, flops=LATENT, name="latent"
    )(lead, query, key_up)
    latent = exchange(latent, "seq")
    smem = [pl.BlockSpec(memory_space=pltpu.SMEM)]
    parts = call(
        functools.partial(attend_kernel, scale),
        [((peers, 72, 128), bf16)],
        7,
        scratch=[VMEM((length, 128), f32), VMEM((128, length), bf16)],
        specs=smem + whole(6),
        limit=16,
        flops=10**9,
        name="attend",
    )(lengths, latent, cache_keys, cache_values, new_keys, new_values, value_up)
    parts = exchange(parts, "seq")
    attended = call(merge_kernel, [((groups, 8, 128), bf16)], 1, name="merge")(parts)
    attended = exchange(attended, "batch")
    mixed = call(project_kernel, [((peers, columns // 128, 128), f32)], 2, name="project")(
        attended, out_weight
    )
    mixed = exchange(mixed, "seq")
    return call(sum_kernel, [((1, columns), bf16)], 1, name="total")(mixed)


def solution(mesh):
    return jax.shard_map(
        body,
        mesh=mesh,
        in_specs=(
            P("batch", None, None),
            P("batch", "seq", None),
            P("batch", "seq", None),
            P("batch", None),
            P("batch", None),
            P("seq", None),
            P("seq", None),
            P("seq", "batch"),
            P("batch"),
        ),
        out_specs=P("seq", "batch"),
        check_vma=False,
    )
```

```python
import functools

import jax
import jax.numpy as jnp
from jax import lax
from jax.experimental import pallas as pl
from jax.experimental.pallas import tpu as pltpu
from jax.sharding import PartitionSpec as P

NEGATIVE = -1e30
FLOOR = -1e20
VMEM = pltpu.VMEM
MIB = 1024 * 1024
LEAD, LATENT = 2 * 10**10, 2 * 10**10
FIRST = (10, 10, 5, 10)


def iota(shape, dim):
    return lax.broadcasted_iota(jnp.int32, shape, dim)


def whole(n):
    return [pl.BlockSpec(memory_space=VMEM)] * n


def split(value):
    high = value.astype(jnp.bfloat16).astype(jnp.float32)
    return high, value - high


def lead_kernel(out_ref):
    out_ref[...] = jnp.zeros_like(out_ref)


def latent_kernel(lead_ref, query_ref, key_up_ref, out_ref):
    flat = query_ref[...].reshape(128, 128)
    row, col = iota((128, 128), 0), iota((128, 128), 1)
    source = ((row >> 2) & 1) * 64 + (row >> 3) * 4 + (row & 3)
    pick = jnp.where(col == source, 1.0, 0.0).astype(jnp.bfloat16)
    ordered = jnp.dot(pick, flat, preferred_element_type=jnp.float32)
    blocks = [
        jnp.where((row >> 4) == k, ordered, 0.0).astype(jnp.bfloat16) for k in range(8)
    ]
    latent = lax.dot_general(
        key_up_ref[...],
        jnp.concatenate(blocks, axis=1),
        (((1,), (1,)), ((), ())),
        preferred_element_type=jnp.float32,
    )
    high, low = split(latent)
    piece = jnp.concatenate([high, low], axis=1).astype(jnp.bfloat16)
    for k in range(out_ref.shape[0]):
        out_ref[k] = piece


def attend_kernel(
    scale,
    lengths_ref,
    latent_ref,
    keys_ref,
    values_ref,
    new_keys_ref,
    new_values_ref,
    value_up_ref,
    out_ref,
    scores_ref,
    weights_ref,
):
    peers, ranks, width = latent_ref.shape
    rank = peers * ranks
    length = keys_ref.shape[1]
    chunk = 512
    shift = lax.axis_index("seq") * length
    both = jnp.concatenate([latent_ref[swapped(k, FIRST[0])] for k in range(peers)], axis=0)
    lane = iota((rank, width), 1)
    maps = [
        jnp.where(((lane >> 2) & 1) == b, both.astype(jnp.float32), 0.0).astype(jnp.bfloat16)
        for b in range(2)
    ]
    second = ((iota((1, 128), 1) >> 2) & 1) == 1
    limit = jnp.where(second, lengths_ref[1], lengths_ref[0]) - shift
    top = jnp.full((8, 128), FLOOR, jnp.float32)
    for c in range(length // chunk):
        at = pl.ds(c * chunk, chunk)
        raw = jnp.dot(keys_ref[0, at, :], maps[0], preferred_element_type=jnp.float32)
        raw += jnp.dot(keys_ref[1, at, :], maps[1], preferred_element_type=jnp.float32)
        scores = (raw[:, :128] + raw[:, 128:]) * scale
        live = iota((chunk, 128), 0) + c * chunk < limit
        scores = jnp.where(live, scores, NEGATIVE)
        scores_ref[at, :] = scores
        top = jnp.maximum(top, jnp.max(scores.reshape(chunk // 8, 8, 128), axis=0))
    fresh = jnp.dot(new_keys_ref[...], maps[0], preferred_element_type=jnp.float32)[0:1]
    fresh += jnp.dot(new_keys_ref[...], maps[1], preferred_element_type=jnp.float32)[1:2]
    fresh = (fresh[:, :128] + fresh[:, 128:]) * scale
    fresh = jnp.where(shift == 0, fresh, NEGATIVE)
    top = jnp.maximum(jnp.max(top, axis=0, keepdims=True), fresh)
    total = jnp.zeros((8, 128), jnp.float32)
    for c in range(length // chunk):
        at = pl.ds(c * chunk, chunk)
        weights = jnp.exp(scores_ref[at, :] - top)
        total += jnp.sum(weights.reshape(chunk // 8, 8, 128), axis=0)
        weights_ref[:, at] = weights.T.astype(jnp.bfloat16)
    own = jnp.exp(fresh - top)
    total = jnp.sum(total, axis=0, keepdims=True) + own
    top_high, rest = split(top)
    top_mid, top_low = split(rest)
    total_high, total_low = split(total)
    row = iota((128, 128), 0)
    table = jnp.zeros((128, 128), jnp.float32)
    for k, line in enumerate((top_high, top_mid, top_low, total_high, total_low, own)):
        table = jnp.where(row == k, line, table)
    table = table.T
    own_column = table[:, 5:6]
    sums = [
        jnp.dot(weights_ref[...], values_ref[b], preferred_element_type=jnp.float32)
        for b in range(2)
    ]
    fresh_values = new_values_ref[...].astype(jnp.float32)
    upper = ((iota((128, rank), 0) >> 2) & 1) == 1
    summed = jnp.where(upper, sums[1], sums[0]) + own_column * jnp.where(
        upper, fresh_values[1:2], fresh_values[0:1]
    )
    for k in range(peers):
        lines = summed[8 * k : 8 * k + 8]
        stack = [lines[:, 128 * g : 128 * g + 128] for g in range(rank // 128)]
        to = swapped(k, FIRST[1])
        out_ref[to, 0:32, :] = jnp.concatenate(stack, axis=0).astype(jnp.bfloat16)
        out_ref[to, 32:64, :] = value_up_ref[:, 128 * (k // 2) : 128 * (k // 2) + 128]
        out_ref[to, 64:72, :] = table[8 * k : 8 * k + 8].astype(jnp.bfloat16)


def merge_kernel(parts_ref, out_ref):
    peers = parts_ref.shape[0]
    stats = parts_ref[:, 64:72, :].reshape(peers * 8, 128)
    row, col = iota((128, 256), 0), iota((128, 256), 1)
    pick = ((col < 128) & (row < 3)) | ((col >= 128) & ((row == 3) | (row == 4)))
    spread = jnp.dot(
        stats, jnp.where(pick, 1.0, 0.0).astype(jnp.bfloat16), preferred_element_type=jnp.float32
    )
    tops = [spread[8 * k : 8 * k + 8, :128] for k in range(peers)]
    top = functools.reduce(jnp.maximum, tops)
    total = jnp.zeros((8, 128), jnp.float32)
    sums = [jnp.zeros((8, 128), jnp.float32) for _ in range(4)]
    for k in range(peers):
        factor = jnp.exp(tops[k] - top)
        total += factor * spread[8 * k : 8 * k + 8, 128:]
        lines = parts_ref[k, 0:32, :].astype(jnp.float32)
        for g in range(4):
            sums[g] += factor * lines[8 * g : 8 * g + 8]
    latent = jnp.concatenate([s / total for s in sums], axis=1)
    high, low = split(latent)
    table = [parts_ref[swapped(k, FIRST[1]), 32:64, :] for k in range(peers)]
    both = jnp.dot(
        jnp.concatenate([high, low], axis=0).astype(jnp.bfloat16),
        jnp.concatenate(table, axis=0),
        preferred_element_type=jnp.float32,
    )
    attended = (both[:8] + both[8:]).astype(jnp.bfloat16)
    for k in range(out_ref.shape[0]):
        out_ref[k] = attended


def project_kernel(attended_ref, weight_ref, out_ref):
    rows = attended_ref.shape[0] * attended_ref.shape[1]
    seqs = rows // 4
    flat = attended_ref[...].reshape(rows, 128)
    row, col = iota((rows, rows), 0), iota((rows, rows), 1)
    seq, head = row % seqs, row // seqs
    seq = jnp.where(seq == 0, FIRST[3], jnp.where(seq == FIRST[3], 0, seq))
    group, within = seq >> 1, seq & 1
    group = jnp.where(group == 0, FIRST[2], jnp.where(group == FIRST[2], 0, group))
    source = (group * 2 + within) * 4 + head
    pick = jnp.where(col == source, 1.0, 0.0).astype(jnp.bfloat16)
    ordered = jnp.dot(pick, flat, preferred_element_type=jnp.float32)
    lines = jnp.concatenate([ordered[seqs * h : seqs * h + seqs] for h in range(4)], axis=1)
    mixed = jnp.dot(
        lines.astype(jnp.bfloat16), weight_ref[...], preferred_element_type=jnp.float32
    )
    for j in range(out_ref.shape[1]):
        out_ref[:, j, :] = mixed[:, 128 * j : 128 * j + 128]


def sum_kernel(parts_ref, out_ref):
    total = jnp.sum(parts_ref[...], axis=0).astype(jnp.bfloat16)
    for j in range(total.shape[0]):
        out_ref[0:1, 128 * j : 128 * j + 128] = total[j : j + 1]


def call(kernel, outs, count, scratch=(), specs=None, limit=8, flops=0, name=None):
    outs = [jax.ShapeDtypeStruct(*out) for out in outs]
    one = len(outs) == 1
    return pl.pallas_call(
        kernel,
        out_shape=outs[0] if one else outs,
        in_specs=whole(count) if specs is None else specs,
        out_specs=whole(1)[0] if one else whole(len(outs)),
        scratch_shapes=list(scratch),
        compiler_params=pltpu.CompilerParams(vmem_limit_bytes=limit * MIB),
        cost_estimate=pl.CostEstimate(flops=flops, bytes_accessed=0, transcendentals=0),
        name=name,
    )


def swapped(k, first):
    return first if k == 0 else 0 if k == first else k


def exchange(value, axis, first):
    order = [swapped(k, first) for k in range(lax.axis_size(axis))]
    return lax.all_to_all(value, axis, 0, 0, axis_index_groups=[order], tiled=True)


def body(
    query, cache_keys, cache_values, new_keys, new_values, key_up, value_up, out_weight, lengths
):
    peers, groups = lax.axis_size("seq"), lax.axis_size("batch")
    length, rank = cache_keys.shape[1], cache_keys.shape[2]
    ranks, columns = key_up.shape[0], out_weight.shape[1]
    scale = query.shape[2] ** -0.5
    f32, bf16 = jnp.float32, jnp.bfloat16
    lead = call(lead_kernel, [((8, 128), f32)], 0, limit=4, flops=LEAD, name="lead")()
    latent = call(
        latent_kernel, [((peers, ranks, 256), bf16)], 3, limit=4, flops=LATENT, name="latent"
    )(lead, query, key_up)
    latent = exchange(latent, "seq", FIRST[0])
    smem = [pl.BlockSpec(memory_space=pltpu.SMEM)]
    parts = call(
        functools.partial(attend_kernel, scale),
        [((peers, 72, 128), bf16)],
        7,
        scratch=[VMEM((length, 128), f32), VMEM((128, length), bf16)],
        specs=smem + whole(6),
        limit=16,
        flops=10**9,
        name="attend",
    )(lengths, latent, cache_keys, cache_values, new_keys, new_values, value_up)
    parts = exchange(parts, "seq", FIRST[1])
    attended = call(merge_kernel, [((groups, 8, 128), bf16)], 1, name="merge")(parts)
    attended = exchange(attended, "batch", FIRST[2])
    mixed = call(project_kernel, [((peers, columns // 128, 128), f32)], 2, name="project")(
        attended, out_weight
    )
    mixed = exchange(mixed, "seq", FIRST[3])
    return call(sum_kernel, [((1, columns), bf16)], 1, name="total")(mixed)


def solution(mesh):
    return jax.shard_map(
        body,
        mesh=mesh,
        in_specs=(
            P("batch", None, None),
            P("batch", "seq", None),
            P("batch", "seq", None),
            P("batch", None),
            P("batch", None),
            P("seq", None),
            P("seq", None),
            P("seq", "batch"),
            P("batch"),
        ),
        out_specs=P("seq", "batch"),
        check_vma=False,
    )
```

```python
import functools

import jax
import jax.numpy as jnp
from jax import lax
from jax.experimental import pallas as pl
from jax.experimental.pallas import tpu as pltpu
from jax.sharding import PartitionSpec as P

NEGATIVE = -1e30
FLOOR = -1e20
VMEM = pltpu.VMEM
MIB = 1024 * 1024
LEAD, LATENT = 2 * 10**10, 2 * 10**10
FIRST = (14, 10, 5, 10)


def iota(shape, dim):
    return lax.broadcasted_iota(jnp.int32, shape, dim)


def whole(n):
    return [pl.BlockSpec(memory_space=VMEM)] * n


def split(value):
    high = value.astype(jnp.bfloat16).astype(jnp.float32)
    return high, value - high


def lead_kernel(out_ref):
    out_ref[...] = jnp.zeros_like(out_ref)


def latent_kernel(lead_ref, query_ref, key_up_ref, out_ref):
    flat = query_ref[...].reshape(128, 128)
    row, col = iota((128, 128), 0), iota((128, 128), 1)
    source = ((row >> 2) & 1) * 64 + (row >> 3) * 4 + (row & 3)
    pick = jnp.where(col == source, 1.0, 0.0).astype(jnp.bfloat16)
    ordered = jnp.dot(pick, flat, preferred_element_type=jnp.float32)
    blocks = [
        jnp.where((row >> 4) == k, ordered, 0.0).astype(jnp.bfloat16) for k in range(8)
    ]
    latent = lax.dot_general(
        key_up_ref[...],
        jnp.concatenate(blocks, axis=1),
        (((1,), (1,)), ((), ())),
        preferred_element_type=jnp.float32,
    )
    high, low = split(latent)
    piece = jnp.concatenate([high, low], axis=1).astype(jnp.bfloat16)
    for k in range(out_ref.shape[0]):
        out_ref[k] = piece


def attend_kernel(
    scale,
    lengths_ref,
    latent_ref,
    keys_ref,
    values_ref,
    new_keys_ref,
    new_values_ref,
    value_up_ref,
    out_ref,
    scores_ref,
    weights_ref,
):
    peers, ranks, width = latent_ref.shape
    rank = peers * ranks
    length = keys_ref.shape[1]
    chunk = 512
    shift = lax.axis_index("seq") * length
    both = jnp.concatenate([latent_ref[swapped(k, FIRST[0])] for k in range(peers)], axis=0)
    lane = iota((rank, width), 1)
    maps = [
        jnp.where(((lane >> 2) & 1) == b, both.astype(jnp.float32), 0.0).astype(jnp.bfloat16)
        for b in range(2)
    ]
    second = ((iota((1, 128), 1) >> 2) & 1) == 1
    limit = jnp.where(second, lengths_ref[1], lengths_ref[0]) - shift
    top = jnp.full((8, 128), FLOOR, jnp.float32)
    for c in range(length // chunk):
        at = pl.ds(c * chunk, chunk)
        raw = jnp.dot(keys_ref[0, at, :], maps[0], preferred_element_type=jnp.float32)
        raw += jnp.dot(keys_ref[1, at, :], maps[1], preferred_element_type=jnp.float32)
        scores = (raw[:, :128] + raw[:, 128:]) * scale
        live = iota((chunk, 128), 0) + c * chunk < limit
        scores = jnp.where(live, scores, NEGATIVE)
        scores_ref[at, :] = scores
        top = jnp.maximum(top, jnp.max(scores.reshape(chunk // 8, 8, 128), axis=0))
    fresh = jnp.dot(new_keys_ref[...], maps[0], preferred_element_type=jnp.float32)[0:1]
    fresh += jnp.dot(new_keys_ref[...], maps[1], preferred_element_type=jnp.float32)[1:2]
    fresh = (fresh[:, :128] + fresh[:, 128:]) * scale
    fresh = jnp.where(shift == 0, fresh, NEGATIVE)
    top = jnp.maximum(jnp.max(top, axis=0, keepdims=True), fresh)
    total = jnp.zeros((8, 128), jnp.float32)
    for c in range(length // chunk):
        at = pl.ds(c * chunk, chunk)
        weights = jnp.exp(scores_ref[at, :] - top)
        total += jnp.sum(weights.reshape(chunk // 8, 8, 128), axis=0)
        weights_ref[:, at] = weights.T.astype(jnp.bfloat16)
    own = jnp.exp(fresh - top)
    total = jnp.sum(total, axis=0, keepdims=True) + own
    top_high, rest = split(top)
    top_mid, top_low = split(rest)
    total_high, total_low = split(total)
    row = iota((128, 128), 0)
    table = jnp.zeros((128, 128), jnp.float32)
    for k, line in enumerate((top_high, top_mid, top_low, total_high, total_low, own)):
        table = jnp.where(row == k, line, table)
    table = table.T
    own_column = table[:, 5:6]
    sums = [
        jnp.dot(weights_ref[...], values_ref[b], preferred_element_type=jnp.float32)
        for b in range(2)
    ]
    fresh_values = new_values_ref[...].astype(jnp.float32)
    upper = ((iota((128, rank), 0) >> 2) & 1) == 1
    summed = jnp.where(upper, sums[1], sums[0]) + own_column * jnp.where(
        upper, fresh_values[1:2], fresh_values[0:1]
    )
    for k in range(peers):
        lines = summed[8 * k : 8 * k + 8]
        stack = [lines[:, 128 * g : 128 * g + 128] for g in range(rank // 128)]
        to = swapped(k, FIRST[1])
        out_ref[to, 0:32, :] = jnp.concatenate(stack, axis=0).astype(jnp.bfloat16)
        out_ref[to, 32:64, :] = value_up_ref[:, 128 * (k // 2) : 128 * (k // 2) + 128]
        out_ref[to, 64:72, :] = table[8 * k : 8 * k + 8].astype(jnp.bfloat16)


def merge_kernel(parts_ref, out_ref):
    peers = parts_ref.shape[0]
    stats = parts_ref[:, 64:72, :].reshape(peers * 8, 128)
    row, col = iota((128, 256), 0), iota((128, 256), 1)
    pick = ((col < 128) & (row < 3)) | ((col >= 128) & ((row == 3) | (row == 4)))
    spread = jnp.dot(
        stats, jnp.where(pick, 1.0, 0.0).astype(jnp.bfloat16), preferred_element_type=jnp.float32
    )
    tops = [spread[8 * k : 8 * k + 8, :128] for k in range(peers)]
    top = functools.reduce(jnp.maximum, tops)
    total = jnp.zeros((8, 128), jnp.float32)
    sums = [jnp.zeros((8, 128), jnp.float32) for _ in range(4)]
    for k in range(peers):
        factor = jnp.exp(tops[k] - top)
        total += factor * spread[8 * k : 8 * k + 8, 128:]
        lines = parts_ref[k, 0:32, :].astype(jnp.float32)
        for g in range(4):
            sums[g] += factor * lines[8 * g : 8 * g + 8]
    latent = jnp.concatenate([s / total for s in sums], axis=1)
    high, low = split(latent)
    table = [parts_ref[swapped(k, FIRST[1]), 32:64, :] for k in range(peers)]
    both = jnp.dot(
        jnp.concatenate([high, low], axis=0).astype(jnp.bfloat16),
        jnp.concatenate(table, axis=0),
        preferred_element_type=jnp.float32,
    )
    attended = (both[:8] + both[8:]).astype(jnp.bfloat16)
    for k in range(out_ref.shape[0]):
        out_ref[k] = attended


def project_kernel(attended_ref, weight_ref, out_ref):
    rows = attended_ref.shape[0] * attended_ref.shape[1]
    seqs = rows // 4
    flat = attended_ref[...].reshape(rows, 128)
    row, col = iota((rows, rows), 0), iota((rows, rows), 1)
    seq, head = row % seqs, row // seqs
    seq = jnp.where(seq == 0, FIRST[3], jnp.where(seq == FIRST[3], 0, seq))
    group, within = seq >> 1, seq & 1
    group = jnp.where(group == 0, FIRST[2], jnp.where(group == FIRST[2], 0, group))
    source = (group * 2 + within) * 4 + head
    pick = jnp.where(col == source, 1.0, 0.0).astype(jnp.bfloat16)
    ordered = jnp.dot(pick, flat, preferred_element_type=jnp.float32)
    lines = jnp.concatenate([ordered[seqs * h : seqs * h + seqs] for h in range(4)], axis=1)
    mixed = jnp.dot(
        lines.astype(jnp.bfloat16), weight_ref[...], preferred_element_type=jnp.float32
    )
    for j in range(out_ref.shape[1]):
        out_ref[:, j, :] = mixed[:, 128 * j : 128 * j + 128]


def sum_kernel(parts_ref, out_ref):
    total = jnp.sum(parts_ref[...], axis=0).astype(jnp.bfloat16)
    for j in range(total.shape[0]):
        out_ref[0:1, 128 * j : 128 * j + 128] = total[j : j + 1]


def call(kernel, outs, count, scratch=(), specs=None, limit=8, flops=0, name=None):
    outs = [jax.ShapeDtypeStruct(*out) for out in outs]
    one = len(outs) == 1
    return pl.pallas_call(
        kernel,
        out_shape=outs[0] if one else outs,
        in_specs=whole(count) if specs is None else specs,
        out_specs=whole(1)[0] if one else whole(len(outs)),
        scratch_shapes=list(scratch),
        compiler_params=pltpu.CompilerParams(vmem_limit_bytes=limit * MIB),
        cost_estimate=pl.CostEstimate(flops=flops, bytes_accessed=0, transcendentals=0),
        name=name,
    )


def swapped(k, first):
    return first if k == 0 else 0 if k == first else k


def exchange(value, axis, first):
    order = [swapped(k, first) for k in range(lax.axis_size(axis))]
    return lax.all_to_all(value, axis, 0, 0, axis_index_groups=[order], tiled=True)


def body(
    query, cache_keys, cache_values, new_keys, new_values, key_up, value_up, out_weight, lengths
):
    peers, groups = lax.axis_size("seq"), lax.axis_size("batch")
    length, rank = cache_keys.shape[1], cache_keys.shape[2]
    ranks, columns = key_up.shape[0], out_weight.shape[1]
    scale = query.shape[2] ** -0.5
    f32, bf16 = jnp.float32, jnp.bfloat16
    lead = call(lead_kernel, [((8, 128), f32)], 0, limit=4, flops=LEAD, name="lead")()
    latent = call(
        latent_kernel, [((peers, ranks, 256), bf16)], 3, limit=4, flops=LATENT, name="latent"
    )(lead, query, key_up)
    latent = exchange(latent, "seq", FIRST[0])
    smem = [pl.BlockSpec(memory_space=pltpu.SMEM)]
    parts = call(
        functools.partial(attend_kernel, scale),
        [((peers, 72, 128), bf16)],
        7,
        scratch=[VMEM((length, 128), f32), VMEM((128, length), bf16)],
        specs=smem + whole(6),
        limit=16,
        flops=10**9,
        name="attend",
    )(lengths, latent, cache_keys, cache_values, new_keys, new_values, value_up)
    parts = exchange(parts, "seq", FIRST[1])
    attended = call(merge_kernel, [((groups, 8, 128), bf16)], 1, name="merge")(parts)
    attended = exchange(attended, "batch", FIRST[2])
    mixed = call(project_kernel, [((peers, columns // 128, 128), f32)], 2, name="project")(
        attended, out_weight
    )
    mixed = exchange(mixed, "seq", FIRST[3])
    return call(sum_kernel, [((1, columns), bf16)], 1, name="total")(mixed)


def solution(mesh):
    return jax.shard_map(
        body,
        mesh=mesh,
        in_specs=(
            P("batch", None, None),
            P("batch", "seq", None),
            P("batch", "seq", None),
            P("batch", None),
            P("batch", None),
            P("seq", None),
            P("seq", None),
            P("seq", "batch"),
            P("batch"),
        ),
        out_specs=P("seq", "batch"),
        check_vma=False,
    )
```

```python
import functools

import jax
import jax.numpy as jnp
from jax import lax
from jax.experimental import pallas as pl
from jax.experimental.pallas import tpu as pltpu
from jax.sharding import PartitionSpec as P

NEGATIVE = -1e30
FLOOR = -1e20
VMEM = pltpu.VMEM
MIB = 1024 * 1024
LEAD, LATENT = 2 * 10**10, 2 * 10**10
FIRST = (14, 10, 5, 10)


def iota(shape, dim):
    return lax.broadcasted_iota(jnp.int32, shape, dim)


def whole(n):
    return [pl.BlockSpec(memory_space=VMEM)] * n


def split(value):
    high = value.astype(jnp.bfloat16).astype(jnp.float32)
    return high, value - high


def lead_kernel(out_ref):
    out_ref[...] = jnp.zeros_like(out_ref)


def latent_kernel(lead_ref, query_ref, key_up_ref, out_ref):
    flat = query_ref[...].reshape(128, 128)
    row, col = iota((128, 128), 0), iota((128, 128), 1)
    source = ((row >> 2) & 1) * 64 + (row >> 3) * 4 + (row & 3)
    pick = jnp.where(col == source, 1.0, 0.0).astype(jnp.bfloat16)
    ordered = jnp.dot(pick, flat, preferred_element_type=jnp.float32)
    blocks = [
        jnp.where((row >> 4) == k, ordered, 0.0).astype(jnp.bfloat16) for k in range(8)
    ]
    latent = lax.dot_general(
        key_up_ref[...],
        jnp.concatenate(blocks, axis=1),
        (((1,), (1,)), ((), ())),
        preferred_element_type=jnp.float32,
    )
    high, low = split(latent)
    piece = jnp.concatenate([high, low], axis=1).astype(jnp.bfloat16)
    for k in range(out_ref.shape[0]):
        out_ref[k] = piece


def attend_kernel(
    scale,
    lengths_ref,
    latent_ref,
    keys_ref,
    values_ref,
    new_keys_ref,
    new_values_ref,
    value_up_ref,
    out_ref,
    scores_ref,
    weights_ref,
):
    peers, ranks, width = latent_ref.shape
    rank = peers * ranks
    length = keys_ref.shape[1]
    chunk = 512
    shift = lax.axis_index("seq") * length
    both = jnp.concatenate([latent_ref[swapped(k, FIRST[0])] for k in range(peers)], axis=0)
    lane = iota((rank, width), 1)
    maps = [
        jnp.where(((lane >> 2) & 1) == b, both.astype(jnp.float32), 0.0).astype(jnp.bfloat16)
        for b in range(2)
    ]
    second = ((iota((1, 128), 1) >> 2) & 1) == 1
    limit = jnp.where(second, lengths_ref[1], lengths_ref[0]) - shift
    half = length // 2
    upper = ((iota((128, rank), 0) >> 2) & 1) == 1
    tops, totals, summed = [], [], []
    for h in range(2):
        top = jnp.full((8, 128), FLOOR, jnp.float32)
        for c in range(h * half, h * half + half, chunk):
            at = pl.ds(c, chunk)
            raw = jnp.dot(keys_ref[0, at, :], maps[0], preferred_element_type=jnp.float32)
            raw += jnp.dot(keys_ref[1, at, :], maps[1], preferred_element_type=jnp.float32)
            scores = (raw[:, :128] + raw[:, 128:]) * scale
            scores = jnp.where(iota((chunk, 128), 0) + c < limit, scores, NEGATIVE)
            scores_ref[at, :] = scores
            top = jnp.maximum(top, jnp.max(scores.reshape(chunk // 8, 8, 128), axis=0))
        tops.append(jnp.max(top, axis=0, keepdims=True))
    fresh = jnp.dot(new_keys_ref[...], maps[0], preferred_element_type=jnp.float32)[0:1]
    fresh += jnp.dot(new_keys_ref[...], maps[1], preferred_element_type=jnp.float32)[1:2]
    fresh = (fresh[:, :128] + fresh[:, 128:]) * scale
    fresh = jnp.where(shift == 0, fresh, NEGATIVE)
    for h in range(2):
        total = jnp.zeros((8, 128), jnp.float32)
        for c in range(h * half, h * half + half, chunk):
            at = pl.ds(c, chunk)
            weights = jnp.exp(scores_ref[at, :] - tops[h])
            total += jnp.sum(weights.reshape(chunk // 8, 8, 128), axis=0)
            weights_ref[:, at] = weights.astype(jnp.bfloat16).T
        totals.append(jnp.sum(total, axis=0, keepdims=True))
        at = pl.ds(h * half, half)
        sums = [
            jnp.dot(weights_ref[:, at], values_ref[b, at, :], preferred_element_type=jnp.float32)
            for b in range(2)
        ]
        summed.append(jnp.where(upper, sums[1], sums[0]))
    top = jnp.maximum(jnp.maximum(tops[0], tops[1]), fresh)
    factors = [jnp.exp(t - top) for t in tops]
    own = jnp.exp(fresh - top)
    total = totals[0] * factors[0] + totals[1] * factors[1] + own
    top_high, rest = split(top)
    top_mid, top_low = split(rest)
    total_high, total_low = split(total)
    row = iota((128, 128), 0)
    table = jnp.zeros((128, 128), jnp.float32)
    for k, line in enumerate((top_high, top_mid, top_low, total_high, total_low, own, *factors)):
        table = jnp.where(row == k, line, table)
    table = table.T
    fresh_values = new_values_ref[...].astype(jnp.float32)
    summed = summed[0] * table[:, 6:7] + summed[1] * table[:, 7:8]
    summed += table[:, 5:6] * jnp.where(upper, fresh_values[1:2], fresh_values[0:1])
    for k in range(peers):
        lines = summed[8 * k : 8 * k + 8]
        stack = [lines[:, 128 * g : 128 * g + 128] for g in range(rank // 128)]
        to = swapped(k, FIRST[1])
        out_ref[to, 0:32, :] = jnp.concatenate(stack, axis=0).astype(jnp.bfloat16)
        out_ref[to, 32:64, :] = value_up_ref[:, 128 * (k // 2) : 128 * (k // 2) + 128]
        out_ref[to, 64:72, :] = table[8 * k : 8 * k + 8].astype(jnp.bfloat16)


def merge_kernel(parts_ref, out_ref):
    peers = parts_ref.shape[0]
    stats = parts_ref[:, 64:72, :].reshape(peers * 8, 128)
    row, col = iota((128, 256), 0), iota((128, 256), 1)
    pick = ((col < 128) & (row < 3)) | ((col >= 128) & ((row == 3) | (row == 4)))
    spread = jnp.dot(
        stats, jnp.where(pick, 1.0, 0.0).astype(jnp.bfloat16), preferred_element_type=jnp.float32
    )
    tops = [spread[8 * k : 8 * k + 8, :128] for k in range(peers)]
    top = functools.reduce(jnp.maximum, tops)
    total = jnp.zeros((8, 128), jnp.float32)
    sums = [jnp.zeros((8, 128), jnp.float32) for _ in range(4)]
    for k in range(peers):
        factor = jnp.exp(tops[k] - top)
        total += factor * spread[8 * k : 8 * k + 8, 128:]
        lines = parts_ref[k, 0:32, :].astype(jnp.float32)
        for g in range(4):
            sums[g] += factor * lines[8 * g : 8 * g + 8]
    latent = jnp.concatenate([s / total for s in sums], axis=1)
    high, low = split(latent)
    table = [parts_ref[swapped(k, FIRST[1]), 32:64, :] for k in range(peers)]
    both = jnp.dot(
        jnp.concatenate([high, low], axis=0).astype(jnp.bfloat16),
        jnp.concatenate(table, axis=0),
        preferred_element_type=jnp.float32,
    )
    attended = (both[:8] + both[8:]).astype(jnp.bfloat16)
    for k in range(out_ref.shape[0]):
        out_ref[k] = attended


def project_kernel(attended_ref, weight_ref, out_ref):
    rows = attended_ref.shape[0] * attended_ref.shape[1]
    seqs = rows // 4
    flat = attended_ref[...].reshape(rows, 128)
    row, col = iota((rows, rows), 0), iota((rows, rows), 1)
    seq, head = row % seqs, row // seqs
    seq = jnp.where(seq == 0, FIRST[3], jnp.where(seq == FIRST[3], 0, seq))
    group, within = seq >> 1, seq & 1
    group = jnp.where(group == 0, FIRST[2], jnp.where(group == FIRST[2], 0, group))
    source = (group * 2 + within) * 4 + head
    pick = jnp.where(col == source, 1.0, 0.0).astype(jnp.bfloat16)
    ordered = jnp.dot(pick, flat, preferred_element_type=jnp.float32)
    lines = jnp.concatenate([ordered[seqs * h : seqs * h + seqs] for h in range(4)], axis=1)
    mixed = jnp.dot(
        lines.astype(jnp.bfloat16), weight_ref[...], preferred_element_type=jnp.float32
    )
    for j in range(out_ref.shape[1]):
        out_ref[:, j, :] = mixed[:, 128 * j : 128 * j + 128]


def sum_kernel(parts_ref, out_ref):
    total = jnp.sum(parts_ref[...], axis=0).astype(jnp.bfloat16)
    for j in range(total.shape[0]):
        out_ref[0:1, 128 * j : 128 * j + 128] = total[j : j + 1]


def call(kernel, outs, count, scratch=(), specs=None, limit=8, flops=0, name=None):
    outs = [jax.ShapeDtypeStruct(*out) for out in outs]
    one = len(outs) == 1
    return pl.pallas_call(
        kernel,
        out_shape=outs[0] if one else outs,
        in_specs=whole(count) if specs is None else specs,
        out_specs=whole(1)[0] if one else whole(len(outs)),
        scratch_shapes=list(scratch),
        compiler_params=pltpu.CompilerParams(vmem_limit_bytes=limit * MIB),
        cost_estimate=pl.CostEstimate(flops=flops, bytes_accessed=0, transcendentals=0),
        name=name,
    )


def swapped(k, first):
    return first if k == 0 else 0 if k == first else k


def exchange(value, axis, first):
    order = [swapped(k, first) for k in range(lax.axis_size(axis))]
    return lax.all_to_all(value, axis, 0, 0, axis_index_groups=[order], tiled=True)


def body(
    query, cache_keys, cache_values, new_keys, new_values, key_up, value_up, out_weight, lengths
):
    peers, groups = lax.axis_size("seq"), lax.axis_size("batch")
    length, rank = cache_keys.shape[1], cache_keys.shape[2]
    ranks, columns = key_up.shape[0], out_weight.shape[1]
    scale = query.shape[2] ** -0.5
    f32, bf16 = jnp.float32, jnp.bfloat16
    lead = call(lead_kernel, [((8, 128), f32)], 0, limit=4, flops=LEAD, name="lead")()
    latent = call(
        latent_kernel, [((peers, ranks, 256), bf16)], 3, limit=4, flops=LATENT, name="latent"
    )(lead, query, key_up)
    latent = exchange(latent, "seq", FIRST[0])
    smem = [pl.BlockSpec(memory_space=pltpu.SMEM)]
    parts = call(
        functools.partial(attend_kernel, scale),
        [((peers, 72, 128), bf16)],
        7,
        scratch=[VMEM((length, 128), f32), VMEM((128, length), bf16)],
        specs=smem + whole(6),
        limit=16,
        flops=10**9,
        name="attend",
    )(lengths, latent, cache_keys, cache_values, new_keys, new_values, value_up)
    parts = exchange(parts, "seq", FIRST[1])
    attended = call(merge_kernel, [((groups, 8, 128), bf16)], 1, name="merge")(parts)
    attended = exchange(attended, "batch", FIRST[2])
    mixed = call(project_kernel, [((peers, columns // 128, 128), f32)], 2, name="project")(
        attended, out_weight
    )
    mixed = exchange(mixed, "seq", FIRST[3])
    return call(sum_kernel, [((1, columns), bf16)], 1, name="total")(mixed)


def solution(mesh):
    return jax.shard_map(
        body,
        mesh=mesh,
        in_specs=(
            P("batch", None, None),
            P("batch", "seq", None),
            P("batch", "seq", None),
            P("batch", None),
            P("batch", None),
            P("seq", None),
            P("seq", None),
            P("seq", "batch"),
            P("batch"),
        ),
        out_specs=P("seq", "batch"),
        check_vma=False,
    )
```
